256 devices in a mesh: groups: 4 (over x, y), seq: 64 (over z, core).
Axes of the slice: x: 2, y: 2, z: 32, core: 2. Of those that a mesh axis runs over, the one named last changes fastest.
The devices are a block of a 4x8x32 slice.
Arguments:
- atoms: bfloat16 [4, 32768, 128], P('groups', 'seq'), parts along dimension 0, may hold values from -6 to 6
- s_cond: bfloat16 [16384, 768], P(('groups', 'seq')), parts along dimension 0, may hold values from -6 to 6
- token_start: int32 [16384], P(('groups', 'seq')), parts along dimension 0, may hold values from 0 to 32767, as said below
- token_len: int32 [16384], P(('groups', 'seq')), parts along dimension 0, may hold values from 1 to 12, as said below
- atom_mask: int32 [131072], P(('groups', 'seq')), parts along dimension 0, may hold values 0 or 1
- atom_bias: float32 [16, 32768, 128], P('groups', 'seq'), parts along dimension 0, may hold values from -4 to 250
- pair_bias: bfloat16 [64, 4096, 4096], P('groups', 'seq'), parts along dimension 0, may hold values from -4 to 250
- atom_proj: bfloat16 [6, 4, 128, 128], replicated, may hold values from -0.5 to 0.5
- atom_up: bfloat16 [6, 2, 128, 256], replicated, may hold values from -0.5 to 0.5
- atom_down: bfloat16 [6, 256, 128], replicated, may hold values from -0.375 to 0.375
- atom_gains: float32 [6, 2, 128], replicated, may hold values from 0.5 to 1.5
- to_token: bfloat16 [128, 768], replicated, may hold values from -0.5 to 0.5
- token_proj: bfloat16 [4, 768, 768], replicated, may hold values from -0.21875 to 0.21875
- token_gain: float32 [768], replicated, may hold values from 0.5 to 2
- to_atom: bfloat16 [768, 128], replicated, may hold values from -0.21875 to 0.21875
Outputs:
- atoms_out: bfloat16 [4, 32768, 128], P('groups', 'seq'), parts along dimension 0
The draws below stay inside these ranges and needn't reach their ends.
There are 4 independent parts, one for each index of `groups`. The reference program is written for one: setup_inputs(seed, part) draws one part's arguments, and reference() takes and returns one part's arrays. A program takes and returns all parts, laid end to end along the dimension named above; an argument that names none is the same for every part. Nothing has to cross between parts.
Inputs may be any that keep to these rules, and one draw needn't show every extreme that they name: Token t lies in block d = t // 64; its atoms token_start[t] .. token_start[t] + token_len[t] - 1 lie within atoms (d - 1) * 512 .. (d + 2) * 512 - 1 and within the complex. Ranges of the tokens of one block are disjoint and rise with t; ranges of different blocks may share atoms; atoms may belong to no token. `token_len`: every block of 64 tokens has a token of exactly 12 atoms.
All inputs are finite; a program needn't handle non-finite values. No bound on the sum of `atom_mask` on one device may be relied on, other than what follows from the above.
Results may differ from the reference program's by a relative error of at most 0.024.
Values may be sent and summed in bfloat16 or wider, within the bound.
No kernel may reach another device: no remote copies, remote signals or barrier semaphores. Data moves between devices by JAX's collectives and lax.ppermute only.
A program may use at most 128 MiB of HBM per device.

```python
import math
import jax
import jax.numpy as jnp
from jax import lax

S = 1
TOK_DEV = 64
MOSTLEN = 12
CA = 128
CT = 768
HT = 16
HA = 4
ATRANS = 256
WQ = 32
WK = 128
ENC_LAYERS = 3
DEC_LAYERS = 3
BLOCKS = 6
AT_DEV = 512
TOKENS = 4096
ATOMS = 32768


def token_ranges(key):
    blocks = TOKENS // TOK_DEV
    lengths = jax.random.randint(jax.random.fold_in(key, 11), (blocks, TOK_DEV), 1, MOSTLEN + 1)
    place = jax.random.randint(jax.random.fold_in(key, 13), (blocks, 1), 0, TOK_DEV)
    lengths = jnp.where(jnp.arange(TOK_DEV)[None, :] == place, MOSTLEN, lengths)
    shifts = jax.random.randint(jax.random.fold_in(key, 12), (blocks,), -(AT_DEV // 2), AT_DEV // 2)
    block_ids = jnp.arange(blocks)
    shifts = jnp.where(block_ids == 0, 0, shifts)
    shifts = jnp.where(block_ids == blocks - 1, -(AT_DEV // 2), shifts)
    inside = jnp.cumsum(lengths, axis=1) - lengths
    starts = block_ids[:, None] * AT_DEV + shifts[:, None] + inside
    return (starts.reshape(-1).astype(jnp.int32), lengths.reshape(-1).astype(jnp.int32))


def biased(key, head_count, row_count, col_count):
    keys_all = jax.random.split(key, 1)
    entries = jnp.clip(jax.random.normal(keys_all[0], (head_count, row_count, col_count), jnp.float32), -4.0, 4.0)
    return entries


def draw_token_start(key, part):
    return token_ranges(key)[0]


def draw_token_len(key, part):
    return token_ranges(key)[1]


def draw_atom_bias(key, part):
    return biased(jax.random.fold_in(key, 21), HA, ATOMS, WK).astype(jnp.float32)


def draw_pair_bias(key, part):
    return biased(jax.random.fold_in(key, 22), HT, TOKENS, TOKENS).astype(jnp.bfloat16)


def touch_ends(values, rng, low, largest):
    spot = [jax.random.randint(jax.random.fold_in(rng, axis), (), 0, length) for axis, length in enumerate(values.shape)]
    main_axis = values.shape.index(max(values.shape))
    beside = spot[:main_axis] + [(spot[main_axis] + 1) % values.shape[main_axis]] + spot[main_axis + 1:]
    return values.at[tuple(spot)].set(low).at[tuple(beside)].set(largest)


def levels(stream_key, dims, shards, least, largest):
    def one(position, parts):
        steps = jax.random.uniform(jax.random.fold_in(jax.random.fold_in(stream_key, 6), position), (parts,), jnp.float32, least / len(shards), largest / len(shards))
        return jnp.repeat(jnp.exp(steps), dims[position] // parts).reshape((-1,) + (1,) * (len(dims) - position - 1))

    loudness = one(*shards[0])
    for cut in shards[1:]:
        loudness = loudness * one(*cut)
    return loudness


def gaussian(stream_key, dims, width, limit, pieces=(), kind=jnp.bfloat16):
    array = width * jax.random.normal(stream_key, dims, jnp.float32)
    if pieces:
        array = array * levels(stream_key, dims, pieces, -0.22, 0.18)
    return jnp.clip(array, -limit, limit).astype(kind)


def setup_inputs(seed: int = 0, part: int = 0) -> dict:
    key_list = jax.random.split(jax.random.key(seed), 16)
    part_keys = jax.random.split(jax.random.fold_in(key_list[15], part), 16)
    atoms = gaussian(part_keys[0], (S, ATOMS, CA), 1.0, 6.0, ((1, 64),))
    s_cond = gaussian(part_keys[1], (TOKENS, CT), 1.0, 6.0, ((0, 64),))
    token_start = draw_token_start(jax.random.fold_in(jax.random.fold_in(key_list[15], part), 71), part)
    token_len = draw_token_len(jax.random.fold_in(jax.random.fold_in(key_list[15], part), 71), part)
    atom_mask = touch_ends((jax.random.randint(part_keys[4], (ATOMS,), 0, 8) < 7).astype(jnp.int32), jax.random.fold_in(part_keys[4], 1), 0, 1)
    atom_bias = draw_atom_bias(jax.random.fold_in(jax.random.fold_in(key_list[15], part), 71), part)
    pair_bias = draw_pair_bias(jax.random.fold_in(jax.random.fold_in(key_list[15], part), 71), part)
    atom_proj = gaussian(key_list[7], (BLOCKS, 4, CA, CA), CA ** -0.5, 0.5)
    atom_up = gaussian(key_list[8], (BLOCKS, 2, CA, ATRANS), CA ** -0.5, 0.5)
    atom_down = gaussian(key_list[9], (BLOCKS, ATRANS, CA), ATRANS ** -0.5, 0.375)
    atom_gains = jnp.clip(1.0 + 0.1 * jax.random.normal(key_list[10], (BLOCKS, 2, CA), jnp.float32), 0.5, 1.5)
    to_token = gaussian(key_list[11], (CA, CT), CA ** -0.5, 0.5)
    token_proj = gaussian(key_list[12], (4, CT, CT), CT ** -0.5, 0.21875)
    token_gain = jnp.clip(jnp.exp(jax.random.uniform(key_list[13], (CT,), jnp.float32, math.log(0.5), math.log(2.0))), 0.5, 2.0)
    to_atom = gaussian(key_list[14], (CT, CA), CT ** -0.5, 0.21875)
    return dict(atoms=atoms, s_cond=s_cond, token_start=token_start, token_len=token_len, atom_mask=atom_mask, atom_bias=atom_bias, pair_bias=pair_bias, atom_proj=atom_proj, atom_up=atom_up, atom_down=atom_down, atom_gains=atom_gains, to_token=to_token, token_proj=token_proj, token_gain=token_gain, to_atom=to_atom)


epsilon = 1e-05
masked = -1000000000.0

def layer_norm(values, gain_vec):
    average = lax.optimization_barrier(jnp.mean(values, axis=-1, keepdims=True))
    centred = values - average
    spread = lax.optimization_barrier(jnp.mean(centred * centred, axis=-1, keepdims=True))
    return centred * lax.rsqrt(spread + epsilon) * gain_vec

def atom_block(stream, key_mask, bias_rows, proj_set, up_pair, down_proj, gain_pair):
    samples, atoms_all, channels = stream.shape
    rim = (WK - WQ) // 2
    head_size = channels // HA
    windows = atoms_all // WQ
    normed = layer_norm(stream, gain_pair[0]).astype(jnp.bfloat16)
    queries = jnp.dot(normed, proj_set[0], preferred_element_type=jnp.float32).astype(jnp.bfloat16)
    key_rows = jnp.dot(normed, proj_set[1], preferred_element_type=jnp.float32).astype(jnp.bfloat16)
    value_rows = jnp.dot(normed, proj_set[2], preferred_element_type=jnp.float32).astype(jnp.bfloat16)
    padded_keys = jnp.pad(key_rows, ((0, 0), (rim, rim), (0, 0)))
    padded_values = jnp.pad(value_rows, ((0, 0), (rim, rim), (0, 0)))
    key_index = (jnp.arange(windows, dtype=jnp.int32) * WQ)[:, None] + jnp.arange(WK, dtype=jnp.int32)[None, :]
    window_mask = jnp.pad(key_mask, (rim, rim))[key_index]
    query_win = queries.reshape(samples, windows, WQ, HA, head_size).astype(jnp.float32)
    keys_win = padded_keys[:, key_index].reshape(samples, windows, WK, HA, head_size).astype(jnp.float32)
    values_win = padded_values[:, key_index].reshape(samples, windows, WK, HA, head_size).astype(jnp.float32)
    scores = jnp.einsum('snqhd,snkhd->snhqk', query_win, keys_win)
    bias_terms = bias_rows.reshape(HA, windows, WQ, WK).transpose(1, 0, 2, 3)[None]
    logits = scores * head_size ** (-0.5) + bias_terms + jnp.where(window_mask == 1, 0.0, masked)[None, :, None, None, :]
    weights = jax.nn.softmax(logits, axis=-1).astype(jnp.bfloat16)
    mixture = jnp.einsum('snhqk,snkhd->snqhd', weights.astype(jnp.float32), values_win)
    mixture = mixture.astype(jnp.bfloat16).reshape(samples, atoms_all, channels)
    stream = stream + jnp.dot(mixture, proj_set[3], preferred_element_type=jnp.float32)
    second = layer_norm(stream, gain_pair[1]).astype(jnp.bfloat16)
    gated = jax.nn.silu(jnp.dot(second, up_pair[0], preferred_element_type=jnp.float32))
    hidden = (gated * jnp.dot(second, up_pair[1], preferred_element_type=jnp.float32)).astype(jnp.bfloat16)
    return stream + jnp.dot(hidden, down_proj, preferred_element_type=jnp.float32)

def block_members(block_id, token_start, token_len):
    window = 3 * AT_DEV
    first_atom = jnp.clip((block_id - 1) * AT_DEV, 0, ATOMS - window).astype(jnp.int32)
    starts = lax.dynamic_slice_in_dim(token_start, (block_id * TOK_DEV).astype(jnp.int32), TOK_DEV)
    lengths = lax.dynamic_slice_in_dim(token_len, (block_id * TOK_DEV).astype(jnp.int32), TOK_DEV)
    positions = first_atom + jnp.arange(window, dtype=jnp.int32)
    member = (positions[None, :] >= starts[:, None]) & (positions[None, :] < (starts + lengths)[:, None])
    return (first_atom, member.astype(jnp.float32), lengths)

def reference(atoms, s_cond, token_start, token_len, atom_mask, atom_bias, pair_bias, atom_proj, atom_up, atom_down, atom_gains, to_token, token_proj, token_gain, to_atom):
    stream = atoms.astype(jnp.float32)
    for block_id in range(ENC_LAYERS):
        stream = atom_block(stream, atom_mask, atom_bias, atom_proj[block_id], atom_up[block_id], atom_down[block_id], atom_gains[block_id])
    encoded = stream.astype(jnp.bfloat16)
    window = 3 * AT_DEV
    block_count = TOKENS // TOK_DEV

    def pool_block(block_id):
        block_id = block_id.astype(jnp.int32)
        first_atom, member, lengths = block_members(block_id, token_start, token_len)
        part_atoms = lax.dynamic_slice_in_dim(encoded, first_atom, window, 1)
        projected = jax.nn.relu(jnp.dot(part_atoms, to_token, preferred_element_type=jnp.float32)).astype(jnp.bfloat16)
        totals = jnp.einsum('ta,sac->stc', member, projected.astype(jnp.float32))
        return totals / lengths[None, :, None].astype(jnp.float32)
    pooled = lax.map(pool_block, jnp.arange(block_count, dtype=jnp.int32))
    features = pooled.transpose(1, 0, 2, 3).reshape(S, TOKENS, CT) + s_cond.astype(jnp.float32)[None]
    normed = layer_norm(features, token_gain).astype(jnp.bfloat16)
    queries = jnp.dot(normed, token_proj[0], preferred_element_type=jnp.float32).astype(jnp.bfloat16)
    key_rows = jnp.dot(normed, token_proj[1], preferred_element_type=jnp.float32).astype(jnp.bfloat16)
    value_rows = jnp.dot(normed, token_proj[2], preferred_element_type=jnp.float32).astype(jnp.bfloat16)
    head_size = CT // HT

    def attend(sample_rows):
        query_one, key_one, value_one = sample_rows
        query_h = query_one.reshape(TOKENS, HT, head_size).astype(jnp.float32).transpose(1, 0, 2)
        key_h = key_one.reshape(TOKENS, HT, head_size).astype(jnp.float32).transpose(1, 0, 2)
        value_h = value_one.reshape(TOKENS, HT, head_size).astype(jnp.float32).transpose(1, 0, 2)

        def one_head(head_rows):
            query_x, key_x, value_x, bias_x = head_rows
            scores = jnp.dot(query_x, key_x.T)
            logits = scores * head_size ** (-0.5) + bias_x.astype(jnp.float32)
            weights = jax.nn.softmax(logits, axis=-1).astype(jnp.bfloat16)
            return jnp.dot(weights.astype(jnp.float32), value_x)
        mixture = lax.map(one_head, (query_h, key_h, value_h, pair_bias))
        return mixture.transpose(1, 0, 2).astype(jnp.bfloat16).reshape(TOKENS, CT)
    token_mix = lax.map(attend, (queries, key_rows, value_rows))
    updated = features + jnp.dot(token_mix, token_proj[3], preferred_element_type=jnp.float32)
    atom_rows = jnp.dot(updated.astype(jnp.bfloat16), to_atom, preferred_element_type=jnp.float32).astype(jnp.bfloat16)

    def spread_block(block_id, running):
        block_id = jnp.asarray(block_id).astype(jnp.int32)
        first_atom, member, lengths = block_members(block_id, token_start, token_len)
        rows_block = lax.dynamic_slice_in_dim(atom_rows, (block_id * TOK_DEV).astype(jnp.int32), TOK_DEV, 1)
        contrib = jnp.einsum('ta,stc->sac', member, rows_block.astype(jnp.float32))
        current = lax.dynamic_slice_in_dim(running, first_atom, window, 1)
        return lax.dynamic_update_slice_in_dim(running, current + contrib, first_atom, 1)
    returned = lax.fori_loop(0, block_count, spread_block, jnp.zeros((S, ATOMS, CA), jnp.float32))
    stream = stream + returned
    for block_id in range(ENC_LAYERS, ENC_LAYERS + DEC_LAYERS):
        stream = atom_block(stream, atom_mask, atom_bias, atom_proj[block_id], atom_up[block_id], atom_down[block_id], atom_gains[block_id])
    return stream.astype(jnp.bfloat16)
```

```python
import functools

import jax
import jax.numpy as jnp
from jax import lax
from jax.experimental import pallas as pl
from jax.experimental.pallas import tpu as pltpu
from jax.sharding import PartitionSpec as P


HT = 16
HA = 4
WQ = 32
WK = 128
LAYERS = 3
RIM = (WK - WQ) // 2
STEP = 64
WIDE = LAYERS * STEP
SIDE = WIDE - STEP
GROUP = 8
ROWS = 256
CODES = 16

epsilon = 1e-05
masked = -1000000000.0

f32 = jnp.float32
bf16 = jnp.bfloat16

whole = pl.BlockSpec(memory_space=pltpu.VMEM)
scalars = pl.BlockSpec(memory_space=pltpu.SMEM)
in_place = pl.BlockSpec(memory_space=pl.ANY)
params = pltpu.CompilerParams(vmem_limit_bytes=56 * 1024 * 1024)


def dot(a, b):
    return jnp.dot(a, b, preferred_element_type=f32)


def dot_t(a, b):
    return lax.dot_general(a, b, (((1,), (1,)), ((), ())), preferred_element_type=f32)


def layer_norm(values, gain_vec):
    average = jnp.mean(values, axis=-1, keepdims=True)
    centred = values - average
    spread = jnp.mean(centred * centred, axis=-1, keepdims=True)
    return centred * lax.rsqrt(spread + epsilon) * gain_vec


def chunks(start, stop, size):
    return [(at, min(size, stop - at)) for at in range(start, stop, size)]


def atom_stack(place, key_mask, side_l, bias_m, side_r, proj, up, down, gains, x, qkv, mix):
    rows_all, channels = x.shape
    own = rows_all - 2 * WIDE
    head = channels // HA
    scale = head ** (-0.5)
    lane_head = lax.broadcasted_iota(jnp.int32, (WQ, channels), 1) // head
    at, last = place[0], place[1] - 1

    def attend_windows(entries):
        logits = []
        for first, bias_ref, bias_row, mask_row in entries:
            q = qkv[0, pl.ds(first, WQ), :]
            keys = qkv[1, pl.ds(first - RIM, WK), :]
            zero = jnp.zeros_like(q)
            spread = jnp.concatenate([jnp.where(lane_head == h, q, zero) for h in range(HA)], axis=0)
            bias = jnp.concatenate([bias_ref(h, bias_row) for h in range(HA)], axis=0)
            logits.append(dot_t(spread, keys) * scale + bias + key_mask[pl.ds(mask_row, 1), :])
        logits = jnp.concatenate(logits, axis=0)
        e = jnp.exp(logits - jnp.max(logits, axis=-1, keepdims=True))
        weights = (e * (1.0 / jnp.sum(e, axis=-1, keepdims=True))).astype(bf16)
        outs = []
        for n, (first, _, _, _) in enumerate(entries):
            values = qkv[2, pl.ds(first - RIM, WK), :]
            outs.append(dot(weights[n * HA * WQ : (n + 1) * HA * WQ], values))
        for out, (first, _, _, _) in zip(outs, entries):
            kept = out[:WQ]
            for h in range(1, HA):
                kept = jnp.where(lane_head == h, out[h * WQ : (h + 1) * WQ], kept)
            mix[pl.ds(first, WQ), :] = kept.astype(bf16)

    def left(h, row):
        return side_l[pl.ds(h * SIDE + row, WQ), :]

    def middle_bias(h, row):
        return bias_m[h, pl.ds(row, WQ), :]

    def right(h, row):
        return side_r[pl.ds(h * SIDE + row, WQ), :]

    for layer in range(LAYERS):
        low = layer * STEP
        high = rows_all - low
        if layer:
            x[low:WIDE, :] = jnp.where(at > 0, x[low:WIDE, :], 0.0)
            x[WIDE + own : high, :] = jnp.where(at < last, x[WIDE + own : high, :], 0.0)
        for row, size in chunks(low, high, ROWS):
            normed = layer_norm(x[row : row + size, :], gains[layer, 0:1, :]).astype(bf16)
            for part in range(3):
                qkv[part, row : row + size, :] = dot(normed, proj[layer, part]).astype(bf16)
        extra = SIDE - low
        skip = SIDE - extra
        sides = [
            (low + STEP + w * WQ, left, skip + w * WQ, skip // WQ + w) for w in range(extra // WQ)
        ]
        sides += [
            (WIDE + own + w * WQ, right, w * WQ, (SIDE + own) // WQ + w)
            for w in range(extra // WQ)
        ]
        if sides:
            attend_windows(sides)

        def middle(group, _):
            entries = []
            for w in range(GROUP):
                row = pl.multiple_of((group * GROUP + w) * WQ, WQ)
                entries.append((WIDE + row, middle_bias, row, SIDE // WQ + group * GROUP + w))
            attend_windows(entries)
            return 0

        lax.fori_loop(0, own // WQ // GROUP, middle, 0)
        for row, size in chunks(low + STEP, high - STEP, ROWS):
            part = slice(row, row + size)
            first = x[part, :] + dot(mix[part, :], proj[layer, 3])
            second = layer_norm(first, gains[layer, 1:2, :]).astype(bf16)
            gate = dot(second, up[layer, 0])
            hidden = (gate * jax.nn.sigmoid(gate) * dot(second, up[layer, 1])).astype(bf16)
            x[part, :] = first + dot(hidden, down[layer])


def encode_kernel(
    place, side_l, xm, side_r, key_mask, bm, proj, up, down, gains, out, out16, x, qkv, mix
):
    own = xm.shape[0]
    at = HA * SIDE
    x[0:WIDE, :] = side_l[at : at + WIDE, :]
    x[WIDE : WIDE + own, :] = xm[...].astype(f32)
    x[WIDE + own :, :] = side_r[at : at + WIDE, :]
    atom_stack(place, key_mask, side_l, bm, side_r, proj, up, down, gains, x, qkv, mix)
    done = x[WIDE : WIDE + own, :]
    out[...] = done
    out16[...] = done.astype(bf16)


def decode_kernel(
    place, el, xm, er, r0, r1, r2, r3, r4, side_l, side_r, key_mask, bm, proj, up, down, gains,
    out, x, qkv, mix,
):
    own = xm.shape[0]
    tokens = r0.shape[0] - CODES
    x[0:WIDE, :] = el[own - WIDE :, :].astype(f32)
    x[WIDE : WIDE + own, :] = xm[...]
    x[WIDE + own :, :] = er[:WIDE, :].astype(f32)
    for rows in (r0, r1, r2, r3, r4):
        code = rows[tokens:, :].astype(f32).astype(jnp.int32)
        starts = (code[0:1] * 256 + code[1:2])[:, :tokens]
        ends = starts + code[2:3, :tokens]
        for row, size in chunks(0, x.shape[0], ROWS):
            atom = (
                lax.broadcasted_iota(jnp.int32, (size, tokens), 0) + place[0] * own + (row - WIDE)
            )
            member = ((atom >= starts) & (atom < ends)).astype(f32).astype(bf16)
            x[row : row + size, :] += dot(member, rows[:tokens, :])
    atom_stack(place, key_mask, side_l, bm, side_r, proj, up, down, gains, x, qkv, mix)
    out[...] = x[WIDE : WIDE + own, :].astype(bf16)


def pool_kernel(place, el, em, er, to_token, starts, lens, cond, gain, features, normed):
    own = em.shape[0]
    tokens = cond.shape[0]
    begin = starts[...]
    end = begin + lens[...]
    totals = jnp.zeros(cond.shape, f32)
    for k, part in enumerate((el, em, er)):
        projected = jnp.maximum(dot(part[...], to_token[...]), 0.0).astype(bf16)
        atom = lax.broadcasted_iota(jnp.int32, (tokens, own), 1) + (place[0] + (k - 1)) * own
        member = ((atom >= begin) & (atom < end)).astype(f32).astype(bf16)
        totals += dot(member, projected)
    feats = totals / lens[...].astype(f32) + cond[...].astype(f32)
    features[...] = feats
    normed[...] = layer_norm(feats, gain[...]).astype(bf16)


def query_kernel(u, wq, wk, out):
    tokens, width = u.shape
    head = width // HT
    half = width // 2
    scale = head ** (-0.5)
    queries = dot(u[...], wq[0]).astype(bf16)
    lane_head = lax.broadcasted_iota(jnp.int32, (tokens, half), 1) // head
    for side in range(2):
        part = queries[:, side * half : (side + 1) * half]
        zero = jnp.zeros_like(part)
        spread = jnp.concatenate(
            [jnp.where(lane_head == h, part, zero) for h in range(HT // 2)], axis=0
        )
        rows = spread.shape[0]
        out[side * rows : (side + 1) * rows, :] = (
            dot_t(spread, wk[0, :, side * half : (side + 1) * half]) * scale
        ).astype(bf16)


def attend_kernel(first, pieces, *refs):
    if first:
        ids, queries, bias_hbm = refs[:3]
        blocks = refs[3 : 3 + pieces]
        out, top, total, keys, bias, sems = refs[3 + pieces :]
    else:
        ids, queries, bias_hbm, acc_in, top_in, total_in = refs[:6]
        blocks = refs[6 : 6 + pieces]
        out, top, total, keys, bias, sems = refs[6 + pieces :]
    heads, tokens = bias.shape[1:3]
    size = blocks[0].shape[0]
    wide = bias.shape[3]
    chips = bias.shape[0]
    copies = []
    for k in range(chips):
        source = bias_hbm.at[:, :, pl.ds(pl.multiple_of(ids[k] * wide, wide), wide)]
        copies.append(pltpu.make_async_copy(source, bias.at[k], sems.at[k]))
        copies[-1].start()
    for k, block in enumerate(blocks):
        keys[k * size : (k + 1) * size, :] = block[...]
    for copy in copies:
        copy.wait()
    rows = 4 * tokens

    def some_heads(n, _):
        part = pl.ds(pl.multiple_of(n * rows, rows), rows)
        added = jnp.concatenate(
            [bias[k, pl.ds(n * 4, 4)].reshape(rows, wide).astype(f32) for k in range(chips)],
            axis=1,
        )
        logits = dot_t(queries[part, :], keys[...]) + added
        peak = jnp.max(logits, axis=-1, keepdims=True)
        if not first:
            before = top_in[part, 0:1]
            peak = jnp.maximum(peak, before)
        e = jnp.exp(logits - peak)
        summed = jnp.sum(e, axis=-1, keepdims=True)
        mixed = dot(e.astype(bf16), keys[...])
        if not first:
            fade = jnp.exp(before - peak)
            summed += fade * total_in[part, 0:1]
            mixed += fade * acc_in[part, :]
        out[part, :] = mixed
        top[part, :] = jnp.broadcast_to(peak, (rows, 128))
        total[part, :] = jnp.broadcast_to(summed, (rows, 128))
        return 0

    lax.fori_loop(0, heads // 4, some_heads, 0)


def finish_kernel(acc, total, features, wv, wo, to_atom, codes, out):
    tokens, width = features.shape
    head = width // HT
    half = width // 2
    lane_head = lax.broadcasted_iota(jnp.int32, (tokens, half), 1) // head
    count = HT // 2 * tokens
    sides = []
    for side in range(2):
        part = slice(side * count, (side + 1) * count)
        mean = (acc[part, :] * (1.0 / total[part, 0:1])).astype(bf16)
        values = dot(mean, wv[0, :, side * half : (side + 1) * half])
        kept = jnp.zeros((tokens, half), f32)
        for h in range(HT // 2):
            kept = jnp.where(lane_head == h, values[h * tokens : (h + 1) * tokens], kept)
        sides.append(kept.astype(bf16))
    mix = jnp.concatenate(sides, axis=1)
    updated = features[...] + dot(mix, wo[0])
    out[:tokens, :] = dot(updated.astype(bf16), to_atom[...]).astype(bf16)
    out[tokens:, :] = codes[...]


def shape(dims, kind):
    return jax.ShapeDtypeStruct(dims, kind)


def step(
    atoms,
    s_cond,
    token_start,
    token_len,
    atom_mask,
    atom_bias,
    pair_bias,
    atom_proj,
    atom_up,
    atom_down,
    atom_gains,
    to_token,
    token_proj,
    token_gain,
    to_atom,
):
    count = lax.axis_size("seq")
    at = lax.axis_index("seq").astype(jnp.int32)
    place = jnp.stack([at, jnp.full_like(at, count)])
    _, own, channels = atoms.shape
    tokens, width = s_cond.shape

    def from_left(value, far=1):
        return lax.ppermute(value, "seq", [(i, i + far) for i in range(count - far)])

    def from_right(value, far=1):
        return lax.ppermute(value, "seq", [(i + far, i) for i in range(count - far)])

    x = atoms[0]
    lines = WIDE + channels - 1
    lines -= lines % channels

    def packed(bias_part, x_part, mask_part):
        parts = [bias_part.reshape(HA * SIDE, WK), x_part.astype(f32)]
        parts.append(mask_part.astype(f32).reshape(-1, channels))
        return jnp.concatenate(parts, axis=0)

    side_l = from_left(packed(atom_bias[:, own - SIDE :], x[own - WIDE :], atom_mask[own - lines :]))
    side_r = from_right(packed(atom_bias[:, :SIDE], x[:WIDE], atom_mask[:lines]))
    mask_at = HA * SIDE + WIDE
    mask_wide = jnp.concatenate(
        [
            side_l[mask_at:].reshape(-1)[lines - WIDE :],
            atom_mask.astype(f32),
            side_r[mask_at:].reshape(-1)[:WIDE],
        ]
    )
    codes = jnp.zeros((CODES, channels), bf16)
    for k, line in enumerate((token_start // 256, token_start % 256, token_len)):
        codes = codes.at[k, :tokens].set(line.astype(bf16))
    skip = WIDE - SIDE - RIM
    windows = (own + 2 * SIDE) // WQ
    strips = mask_wide[skip : skip + (windows + WK // WQ - 1) * WQ].reshape(-1, WQ)
    key_mask = jnp.where(
        jnp.concatenate([strips[k : k + windows] for k in range(WK // WQ)], axis=1) == 1.0,
        0.0,
        masked,
    ).astype(f32)

    wide = own + 2 * WIDE
    scratch = [
        pltpu.VMEM((wide, channels), f32),
        pltpu.VMEM((3, wide, channels), bf16),
        pltpu.VMEM((wide, channels), bf16),
    ]

    def full(value):
        return pl.BlockSpec(value.shape, lambda i: (0,) * value.ndim)

    def stack_specs(side):
        return [
            pl.BlockSpec((LAYERS,) + w.shape[1:], lambda i, n=w.ndim: (side,) + (0,) * (n - 1))
            for w in (atom_proj, atom_up, atom_down, atom_gains)
        ]

    own_spec = pl.BlockSpec((own, channels), lambda i: (0, 0))
    weights = (atom_proj, atom_up, atom_down, atom_gains)
    ins = (side_l, x, side_r, key_mask, atom_bias)
    encoded, encoded16 = pl.pallas_call(
        encode_kernel,
        grid=(1,),
        in_specs=[scalars] + [full(a) for a in ins] + stack_specs(0),
        out_specs=[own_spec, own_spec],
        out_shape=[shape((own, channels), f32), shape((own, channels), bf16)],
        scratch_shapes=scratch,
        compiler_params=params,
        name="encode",
    )(place, *ins, *weights)

    el = from_left(encoded16)
    er = from_right(encoded16)
    features, normed = pl.pallas_call(
        pool_kernel,
        in_specs=[scalars] + [whole] * 8,
        out_specs=[whole, whole],
        out_shape=[shape((tokens, width), f32), shape((tokens, width), bf16)],
        compiler_params=params,
        name="pool",
    )(
        place, el, encoded16, er, to_token, token_start[:, None], token_len[:, None], s_cond,
        token_gain[None],
    )

    def token_map(which):
        return pl.BlockSpec((1, width, width), lambda i: (which, 0, 0))

    queries = pl.pallas_call(
        query_kernel,
        grid=(1,),
        in_specs=[full(normed), token_map(0), token_map(1)],
        out_specs=pl.BlockSpec((HT * tokens, width), lambda i: (0, 0)),
        out_shape=shape((HT * tokens, width), bf16),
        compiler_params=params,
        name="queries",
    )(normed, token_proj, token_proj)

    chips = count // 2
    core = at % 2
    chip = at // 2
    partner = [(i, i ^ 1) for i in range(count)]
    ring = [(2 * z, 2 * ((z + 1) % chips)) for z in range(chips)]
    ring += [(2 * z + 1, 2 * ((z - 1) % chips) + 1) for z in range(chips)]
    other = lax.ppermute(normed, "seq", partner)
    pair = [jnp.where(core == 0, normed, other), jnp.where(core == 0, other, normed)]
    away = 2 * core - 1
    blocks, order = [pair], [chip]
    ready = [([pair], [chip])]
    moving = pair
    for hop in range(1, chips // 2 + 1):
        first_half = lax.ppermute(moving[0], "seq", ring)
        moving = [first_half, lax.ppermute(moving[1], "seq", ring)]
        blocks, order = [moving], [(chip + hop * away) % chips]
        if hop < chips - hop:
            blocks.append([lax.ppermute(b, "seq", partner) for b in moving])
            order.append((chip - hop * away) % chips)
        ready.append((blocks, order))
    last = ready.pop()
    ready[-1] = (ready[-1][0] + last[0], ready[-1][1] + last[1])

    state = ()
    for blocks, order in ready:
        group = [b for two in blocks for b in two]
        ids = jnp.stack(order).astype(jnp.int32)
        size = len(order)
        carried = len(state)
        dims = [((HT * tokens, width), f32), ((HT * tokens, 128), f32), ((HT * tokens, 128), f32)]
        state = pl.pallas_call(
            functools.partial(attend_kernel, not state, len(group)),
            in_specs=[scalars, whole, in_place] + [whole] * (carried + len(group)),
            out_specs=[whole] * 3,
            out_shape=[shape(*d) for d in dims],
            scratch_shapes=[
                pltpu.VMEM((size * 2 * tokens, width), bf16),
                pltpu.VMEM((size, HT, tokens, 2 * tokens), bf16),
                pltpu.SemaphoreType.DMA((size,)),
            ],
            input_output_aliases={3 + k: k for k in range(carried)},
            compiler_params=params,
            name="attend",
        )(ids, queries, pair_bias, *state, *group)

    acc, _, total = state
    rows = pl.pallas_call(
        finish_kernel,
        grid=(1,),
        in_specs=[full(acc), full(total), full(features), token_map(2), token_map(3),
                  full(to_atom), full(codes)],
        out_specs=pl.BlockSpec((tokens + CODES, channels), lambda i: (0, 0)),
        out_shape=shape((tokens + CODES, channels), bf16),
        compiler_params=params,
        name="finish",
    )(acc, total, features, token_proj, token_proj, to_atom, codes)

    spread = [from_left(rows, 2), from_left(rows), rows, from_right(rows), from_right(rows, 2)]
    ins = (el, encoded, er, *spread, side_l, side_r, key_mask, atom_bias)
    out = pl.pallas_call(
        decode_kernel,
        grid=(1,),
        in_specs=[scalars] + [full(a) for a in ins] + stack_specs(1),
        out_specs=own_spec,
        out_shape=shape((own, channels), bf16),
        scratch_shapes=scratch,
        compiler_params=params,
        name="decode",
    )(place, *ins, *weights)
    return out[None]


def solution(mesh):
    placed = (
        P("groups", "seq", None),
        P(("groups", "seq"), None),
        P(("groups", "seq")),
        P(("groups", "seq")),
        P(("groups", "seq")),
        P("groups", "seq", None),
        P("groups", "seq", None),
        P(),
        P(),
        P(),
        P(),
        P(),
        P(),
        P(),
        P(),
    )
    return jax.shard_map(
        step, mesh=mesh, in_specs=placed, out_specs=P("groups", "seq", None), check_vma=False
    )
```
